32 devices in a mesh: slab: 4 (over y, x), sta: 8 (over z, core).
Axes of the slice: x: 2, y: 2, z: 4, core: 2. Of those that a mesh axis runs over, the one named last changes fastest.
Arguments:
- station_place: float32 [32, 2], P('sta'), may hold values from 0 to 1
- station_height: float32 [32], P('sta'), may hold values from 2 to 8
- cell_weight: float32 [256, 256, 64], P('slab'), may hold values from 0.5 to 2
- kept: int32 [4, 32, 16], P('slab', 'sta'), may hold values from 0 to 8191, as said below
- dest: int32 [4, 32, 16, 1], P('slab', 'sta'), may hold values from 0 to 7; in each aligned block of 64 rows (0 to 63, 64 to 127, ..., all dimensions but the last counted through in order) at most 24 rows name the same one
Outputs:
- owned_blocks: float32 [4, 8, 8, 24, 128], P('slab', 'sta')
The draws below stay inside these ranges and needn't reach their ends.
Inputs may be any that keep to these rules, and one draw needn't show every extreme that they name: `dest`: in the rows of one device (aligned blocks of 64 rows, in order), each owner is named by at most 24 rows, a bound that some block reaches. Let a = k // (256 / (2 * 4)) for a kept id k, and let x-slab p hold x from p * 256 / 4 on, 256 / 4 of them. When a >= 4, the cells on which row a of H(256) is nonzero lie in one x-slab. Among the 64 ids of one y-slab and one index of sta, at most 32 ids with a >= 4 touch any one x-slab, and some x-slab is touched by exactly 32.
All inputs are finite; a program needn't handle non-finite values.
Results may differ from the reference program's by a relative error of at most 0.0003.
Values sent between devices are 32-bit elements; how exact they have to be, the bound alone decides.
A program may use at most 128 MiB of HBM per device.

```python
import math
import jax
import jax.numpy as jnp
import numpy as np
from jax import lax

NX = 256
NY = 256
NZ = 64
STA_DEV = 4
KEEP = 16
STATIONS = 32
CAP = 24
N_SLAB = 4
N_STA = 8


def fine_row(slab, chosen):
    x_local = NX // N_SLAB
    result = jnp.zeros_like(chosen)
    base = 0
    width = 2
    while width <= x_local:
        count = x_local // width
        inside = (chosen >= base) & (chosen < base + count)
        result = jnp.where(inside, NX // width + slab * count + chosen - base, result)
        base = base + count
        width = width * 2
    return result


def draw_kept(key, part):
    rows = STA_DEV * KEEP
    half = NY // N_SLAB // 2
    x_local = NX // N_SLAB
    limit = max(2, 2 * rows // N_SLAB)
    classes = N_SLAB + 1

    def one_group(sub):
        keys = jax.random.split(sub, 6)
        full_slab = jax.random.randint(keys[0], (), 0, N_SLAB)
        shuffled = jax.random.permutation(keys[1], classes * limit)
        class_of = (shuffled // limit).astype(jnp.int32)
        score = jnp.where(class_of == full_slab, 0, 1 + jnp.arange(classes * limit, dtype=jnp.int32))
        ordered = class_of[jnp.argsort(score, stable=True)]
        taken = jax.random.permutation(keys[2], ordered[:rows])
        chosen = jax.random.randint(keys[3], (rows,), 0, x_local - 1)
        fine = fine_row(jnp.minimum(taken, N_SLAB - 1), chosen)
        coarse = jax.random.randint(keys[4], (rows,), 0, N_SLAB)
        xrows = jnp.where(taken == N_SLAB, coarse, fine)
        pairs = jax.random.randint(keys[5], (rows,), 0, half)
        return (xrows * half + pairs).astype(jnp.int32)
    groups = jax.random.split(jax.random.fold_in(key, 71), N_SLAB * N_STA)
    table = jax.vmap(one_group)(groups)
    return table.reshape(N_SLAB, N_STA * STA_DEV, KEEP)


def levels(own_key, extent, pieces, least, high):
    def one(dim, parts):
        draws = jax.random.uniform(jax.random.fold_in(jax.random.fold_in(own_key, 6), dim), (parts,), jnp.float32, least / len(pieces), high / len(pieces))
        return jnp.repeat(jnp.exp(draws), extent[dim] // parts).reshape((-1,) + (1,) * (len(extent) - dim - 1))

    level = one(*pieces[0])
    for cut in pieces[1:]:
        level = level * one(*cut)
    return level


def shared_out(key, own, number, rows, number_of, top, reach, skew):
    ranking = jax.random.permutation(key, number_of)
    packed, common = load_shares(number_of, rows * top, reach, skew, True), load_shares(number_of, rows * top, reach, skew, False)
    places = jnp.arange(number_of)

    def named(lengths, turn):
        used = int((lengths > 0).sum())
        fixed = max(1, used // 4)
        passed = fixed + (places - fixed + turn * (used - fixed)) % max(1, number_of - fixed)
        return jnp.zeros((number_of,), jnp.int32).at[ranking[jnp.where(places < fixed, places, passed)]].set(jnp.asarray(lengths, jnp.int32))

    lengths = jnp.where(number % 4 == 0, named(packed, number // 4), named(common, number - number // 4 - 1))
    mixed = jax.random.permutation(jax.random.fold_in(own, 3), number_of)
    donor, sink = mixed[0:number_of // 2 * 2:2], mixed[1:number_of // 2 * 2:2]
    margin = jnp.minimum(lengths[donor] - 1, reach - lengths[sink]) // 2
    margin = jnp.where((donor == ranking[0]) | (sink == ranking[0]) | (lengths[sink] == 0), 0, jnp.maximum(margin, 0))
    passed = jax.random.randint(jax.random.fold_in(own, 4), (number_of // 2,), 0, 1 << 20) % (margin + 1)
    lengths = lengths.at[donor].add(-passed).at[sink].add(passed)
    members = jnp.searchsorted(jnp.cumsum(lengths), jnp.arange(rows * top), side="right").astype(jnp.int32)
    grid = members.reshape(top, rows).T
    grid = grid[jax.random.permutation(jax.random.fold_in(own, 1), rows)]
    turn = jax.random.randint(jax.random.fold_in(own, 2), (rows, 1), 0, top)
    return jnp.take_along_axis(grid, (jnp.arange(top)[None, :] + turn) % top, axis=1)


def load_shares(number_of, total, most, skew, full):
    weights = [(1 << 20) // math.isqrt(standing ** skew) + 1 for standing in range(1, number_of + 1)]
    largest = most if full else min(most, max(-(-total // number_of), total * weights[0] // sum(weights)))
    least = 1 if total - largest >= number_of - 1 else 0
    holding, surplus = [largest] + [least] * (number_of - 1), total - largest - least * (number_of - 1)
    while surplus > 0:
        free = [i for i in range(1, number_of) if holding[i] < largest] or [i for i in range(1, number_of) if holding[i] < most]
        pool, budget = sum([weights[i] for i in free]), surplus
        for i in free:
            more = min(most - holding[i], max(1, budget * weights[i] // pool), surplus)
            holding[i] = holding[i] + more
            surplus = surplus - more
    return np.array(holding)


def setup_inputs(seed: int = 0) -> dict:
    streams_of = jax.random.split(jax.random.key(seed), 6)
    station_place = jnp.clip(1.0 * jax.random.uniform(streams_of[0], (STATIONS, 2), jnp.float32) ** levels(streams_of[0], (STATIONS, 2), ((0, 8),), -0.2, 0.2), 0.0, 1.0)
    station_height = jnp.clip(jnp.exp(math.log(8.0) - 1.3862944 * jax.random.uniform(streams_of[1], (STATIONS,), jnp.float32) ** levels(streams_of[1], (STATIONS,), ((0, 8),), -0.2, 0.2)), 2.0, 8.0)
    cell_weight = jnp.clip(jnp.exp(math.log(2.0) - 1.3862944 * jax.random.uniform(streams_of[2], (NX, NY, NZ), jnp.float32) ** levels(streams_of[2], (NX, NY, NZ), ((0, 4),), -0.2, 0.2)), 0.5, 2.0)
    kept = draw_kept(jax.random.fold_in(streams_of[5], 71), 0)
    dest_keys = jax.random.split(jax.random.fold_in(streams_of[4], 1), N_SLAB * STATIONS * KEEP // (STA_DEV * KEEP))
    dest_turns = jax.random.permutation(jax.random.fold_in(streams_of[4], 3), N_SLAB * STATIONS * KEEP // (STA_DEV * KEEP))
    dest = jax.vmap(lambda own, number: shared_out(jax.random.fold_in(streams_of[4], 2), own, number, STA_DEV * KEEP, N_STA, 1, CAP, 2))(dest_keys, dest_turns).reshape((N_SLAB, STATIONS, KEEP, 1))
    return dict(station_place=station_place, station_height=station_height, cell_weight=cell_weight, kept=kept, dest=dest)


kernel_scale = 32.0
root_half = 0.7071067811865476

def haar(order):
    matrix = jnp.eye(order, dtype=jnp.float32)
    rows = jnp.arange(order, dtype=jnp.int32)[:, None]
    cols = jnp.arange(order, dtype=jnp.int32)[None, :]
    active = order
    while active % 2 == 0 and active > 1:
        half = active // 2
        low = (rows < half) & ((cols == 2 * rows) | (cols == 2 * rows + 1))
        upper = (rows >= half) & (rows < active)
        plus = upper & (cols == 2 * (rows - half))
        minus = upper & (cols == 2 * (rows - half) + 1)
        keeps = (rows >= active) & (rows == cols)
        step = (jnp.where(low | plus, root_half, 0.0) - jnp.where(minus, root_half, 0.0) + jnp.where(keeps, 1.0, 0.0)).astype(jnp.float32)
        matrix = jnp.dot(step, matrix, precision=lax.Precision.HIGHEST, preferred_element_type=jnp.float32)
        active = half
    return matrix

def kernel(place, height, weight, xs, nx, ny, nz):
    ys = jnp.arange(ny, dtype=jnp.int32).astype(jnp.float32) + 0.5
    zs = jnp.arange(nz, dtype=jnp.int32).astype(jnp.float32) + 0.5
    east = xs[None, :] - place[:, 0:1] * nx
    north = ys[None, :] - place[:, 1:2] * ny
    depth = zs[None, :] + height[:, None]
    radius = east[:, :, None, None] ** 2 + north[:, None, :, None] ** 2 + depth[:, None, None, :] ** 2
    return kernel_scale * weight[None] * depth[:, None, None, :] / (radius * jnp.sqrt(radius))

def reference(station_place, station_height, cell_weight, kept, dest):
    wx, wy, wz = (haar(NX), haar(NY), haar(NZ))
    half = NY // N_SLAB // 2
    xs = jnp.arange(NX, dtype=jnp.int32).astype(jnp.float32) + 0.5
    slabs = jnp.arange(N_SLAB, dtype=jnp.int32)[:, None]

    def one(item):
        place, height, ids = item
        field = kernel(place[None], height[None], cell_weight, xs, NX, NY, NZ)[0]
        field = jnp.einsum('xyz,cz->xyc', field, wz, precision=lax.Precision.HIGHEST)
        field = jnp.einsum('by,xyc->xbc', wy, field, precision=lax.Precision.HIGHEST)
        paired = field.reshape(NX, NY // 2, 2 * NZ)
        xrow = (ids // half).reshape(-1)
        ypair = (slabs * half + ids % half).reshape(-1)
        gathered = paired[:, ypair, :]
        weights = wx[xrow]
        blocks = jnp.einsum('mx,xmc->mc', weights, gathered, precision=lax.Precision.HIGHEST)
        return blocks.reshape(N_SLAB, KEEP, 2 * NZ)
    blocks = lax.map(one, (station_place, station_height, jnp.transpose(kept, (1, 0, 2))))
    per_row = STA_DEV * KEEP
    values = jnp.transpose(blocks, (1, 0, 2, 3)).reshape(N_SLAB, N_STA, per_row, 2 * NZ)
    owner = dest.reshape(N_SLAB, N_STA, per_row)
    owners = jnp.arange(N_STA, dtype=jnp.int32)
    onehot = (owner[..., None] == owners).astype(jnp.int32)
    slot = lax.optimization_barrier(jnp.sum((jnp.cumsum(onehot, axis=2) - onehot) * onehot, axis=3)).astype(jnp.int32)
    slab_ids = jnp.arange(N_SLAB, dtype=jnp.int32)[:, None, None]
    source = jnp.arange(N_STA, dtype=jnp.int32)[None, :, None]
    result = jnp.zeros((N_SLAB, N_STA, N_STA, CAP, 2 * NZ), jnp.float32)
    return result.at[slab_ids, owner, source, slot].set(values)
```

```python
import functools
import math

import jax
import jax.numpy as jnp
from jax import lax
from jax.experimental import pallas as pl
from jax.experimental.pallas import tpu as pltpu
from jax.sharding import PartitionSpec as P

kernel_scale = 32.0
MESH = pl.DeviceIdType.MESH


def log2(n):
    return n.bit_length() - 1


def row_plan(ids, j, me, slab, half, x_cells, y_cells):
    ls = log2(slab)
    a = ids >> log2(half)
    pair = j * half + (ids & (half - 1))
    here = jnp.zeros_like(a)
    factor = jnp.full(a.shape, x_cells ** -0.5, jnp.float32)
    m = 1
    while m < x_cells:
        e = log2(m)
        at = a >= m
        k = a - m
        norm = (m / x_cells) ** 0.5
        if m >= slab:
            sh = e - ls
            mine = (k >> sh) == me
            here = jnp.where(at, (m >> ls) + (k & ((1 << sh) - 1)), here)
            factor = jnp.where(at, jnp.where(mine, norm, 0.0), factor)
        else:
            sh = ls - e
            mine = k == (me >> sh)
            sign = norm * (1 - 2 * ((me >> (sh - 1)) & 1)).astype(jnp.float32)
            factor = jnp.where(at, jnp.where(mine, sign, 0.0), factor)
        m = m * 2
    ynorm = jnp.full(a.shape, y_cells ** -0.5, jnp.float32)
    m = 1
    while m < y_cells // 2:
        ynorm = jnp.where(pair >= m, (2 * m / y_cells) ** 0.5, ynorm)
        m = m * 2
    return here * y_cells + 2 * pair, factor * ynorm


def z_matrix(z_cells, t):
    z = lax.broadcasted_iota(jnp.int32, (2 * z_cells, 2 * z_cells), 0) & (z_cells - 1)
    lane = lax.broadcasted_iota(jnp.int32, (2 * z_cells, 2 * z_cells), 1)
    c = lane & (z_cells - 1)
    value = jnp.full(z.shape, z_cells ** -0.5, jnp.float32)
    m = 1
    while m < z_cells:
        w = log2(z_cells // m)
        k = c - m
        norm = (m / z_cells) ** 0.5
        hit = (z >> w) == k
        up = ((z >> (w - 1)) & 1) == 0
        value = jnp.where(c >= m, jnp.where(hit, jnp.where(up, norm, -norm), 0.0), value)
        m = m * 2
    return jnp.where((lane >> log2(z_cells)) == t, value, 0.0)


def tree(values):
    out = [None] * len(values)
    while len(values) > 1:
        half = len(values) // 2
        for k in range(half):
            out[half + k] = values[2 * k] - values[2 * k + 1]
        values = [values[2 * k] + values[2 * k + 1] for k in range(half)]
    out[0] = values[0]
    return out


GROUP = 4


def local_kernel(sizes, place, height, w_ref, ids_ref, out_ref, field, twice, table, rows_v, rows_s, taken, sem):
    slab, stations, keep, x_local, y_cells, z_cells, chunk = sizes
    lanes = 2 * z_cells
    pairs = stations // 2
    x_cells = x_local * slab
    half = y_cells // slab // 2
    per_row = stations * keep
    runs = y_cells // 8
    step = pl.program_id(0)
    me = lax.axis_index("slab")
    plane = x_local * y_cells
    left = lax.broadcasted_iota(jnp.int32, (8, lanes), 1) < z_cells
    zed = (lax.broadcasted_iota(jnp.int32, (8, lanes), 1) & (z_cells - 1)).astype(jnp.float32) + 0.5

    def two(pair, of):
        return jnp.where(left, of(2 * pair), of(2 * pair + 1))

    depths = [zed + two(p, lambda s: height[s]) for p in range(pairs)]

    @pl.when(step == 0)
    def _():
        for j in range(slab):
            where_from, _ = row_plan(ids_ref[j : j + 1, :], j, me, slab, half, x_cells, y_cells)
            rows_v[j : j + 1, :] = where_from
        copy = pltpu.make_async_copy(rows_v, rows_s, sem)
        copy.start()
        base = (lax.broadcasted_iota(jnp.int32, (8, lanes), 0) * runs).astype(jnp.float32) + 0.5
        for p in range(pairs):
            square = depths[p] * depths[p]
            north = base - two(p, lambda s: place[s, 1] * y_cells)
            for r in range(runs):
                n = north + float(r)
                table[p, r] = n * n + square
        copy.wait()

    first = step * chunk
    for u in range(chunk):
        wide = w_ref[u]
        twice[pl.ds(u * y_cells, y_cells), :] = jnp.concatenate([wide, wide], axis=1)

    def group(g, carry):
        x0 = first + g * GROUP
        for p in range(pairs):
            easts = []
            for u in range(GROUP):
                x = (me * x_local + x0 + u).astype(jnp.float32) + 0.5
                e = x - two(p, lambda s: place[s, 0] * x_cells)
                easts.append(e * e)

            def emit(level, run, values):
                if level is None:
                    start, stride = 0, 1
                else:
                    stride = runs >> level
                    start = (y_cells >> level) + run
                out = tree(values)
                for h in range(GROUP):
                    if h == 0:
                        xrow = x0 // GROUP
                    else:
                        m = 1 << log2(h)
                        xrow = x_local * m // GROUP + (x0 * m // GROUP) + (h - m)
                    at = p * plane + xrow * y_cells + start
                    if stride == 1:
                        field[pl.ds(at, 8), :] = out[h]
                    else:
                        field[pl.ds(at, 8, stride=stride), :] = out[h]

            stack = []
            for r in range(runs):
                t = table[p, r]
                values = []
                for u in range(GROUP):
                    inv = lax.rsqrt(t + easts[u])
                    w = twice[pl.ds((g * GROUP + u) * y_cells + r, 8, stride=runs), :]
                    values.append((w * inv) * (inv * inv))
                level, run = 0, r
                while stack and stack[-1][0] == level:
                    _, other = stack.pop()
                    level, run = level + 1, run >> 1
                    emit(level, run, [o - v for o, v in zip(other, values)])
                    values = [o + v for o, v in zip(other, values)]
                stack.append((level, values))
            emit(None, 0, stack[0][1])
        return carry

    lax.fori_loop(0, chunk // GROUP, group, 0)

    @pl.when(step == pl.num_programs(0) - 1)
    def _():
        coarse = x_local // GROUP

        def finish_x(tile, carry):
            for p in range(pairs):
                at = [p * plane + x * y_cells + tile * 8 for x in range(coarse)]
                values = tree([field[pl.ds(pl.multiple_of(a, 8), 8), :] for a in at])
                for a, v in zip(at, values):
                    field[pl.ds(pl.multiple_of(a, 8), 8), :] = v
            return carry

        lax.fori_loop(0, runs, finish_x, 0)

        def finish_y(block, carry):
            for p in range(pairs):
                at = p * plane + block * (8 * y_cells)
                values = tree([field[pl.ds(at + i, 8, stride=y_cells), :] for i in range(8)])
                for i in range(8):
                    field[pl.ds(at + i, 8, stride=y_cells), :] = values[i]
            return carry

        lax.fori_loop(0, x_local // 8, finish_y, 0)
        even, odd = z_matrix(z_cells, 0), z_matrix(z_cells, 1)
        eye = lax.broadcasted_iota(jnp.int32, (per_row, per_row), 0) == lax.broadcasted_iota(
            jnp.int32, (per_row, per_row), 1
        )
        side = lax.broadcasted_iota(jnp.int32, (1, lanes), 1) < z_cells

        def one_slab(j, carry):
            for s in range(stations):
                for i in range(keep):
                    k = s * keep + i
                    at = (s // 2) * plane + rows_s[j, k]
                    taken[2 * k : 2 * k + 2, :] = field[pl.ds(at, 2), :]
            scales = []
            for s in range(stations):
                d = kernel_scale * depths[s // 2][0:1, :]
                d = jnp.where(side if s % 2 == 0 else jnp.logical_not(side), d, 0.0)
                scales.append(jnp.broadcast_to(d, (keep, lanes)))
            scale = jnp.concatenate(scales, axis=0)
            _, factor = row_plan(ids_ref[pl.ds(j, 1), :], j, me, slab, half, x_cells, y_cells)
            factor = jnp.sum(jnp.where(eye, factor, 0.0), axis=1, keepdims=True)
            scale = scale * factor
            x_even = taken[pl.ds(0, per_row, stride=2), :] * scale
            x_odd = taken[pl.ds(1, per_row, stride=2), :] * scale
            out_ref[j] = jnp.dot(
                x_even, even, precision=lax.Precision.HIGHEST, preferred_element_type=jnp.float32
            ) + jnp.dot(x_odd, odd, precision=lax.Precision.HIGHEST, preferred_element_type=jnp.float32)
            return carry

        lax.fori_loop(0, slab, one_slab, 0)


def send_kernel(sizes, parts, dest, out, arrived, packed, s_send, s_recv, o_send, o_recv, own_sem):
    slab, owners, per_row, capacity = sizes
    me, q = lax.axis_index("slab"), lax.axis_index("sta")
    barrier = pltpu.get_barrier_semaphore()
    for d in range(1, slab):
        to = lax.rem(me + d, slab)
        pl.semaphore_signal(barrier, inc=1, device_id=(to, q), device_id_type=MESH)
    for d in range(1, owners):
        to = lax.rem(q + d, owners)
        pl.semaphore_signal(barrier, inc=1, device_id=(me, to), device_id_type=MESH)
    pl.semaphore_wait(barrier, slab + owners - 2)
    copies = []
    for d in range(1, slab):
        to = lax.rem(me + d, slab)
        copy = pltpu.make_async_remote_copy(
            src_ref=parts.at[to],
            dst_ref=arrived.at[d - 1],
            send_sem=s_send.at[d - 1],
            recv_sem=s_recv.at[d - 1],
            device_id=(to, q),
            device_id_type=MESH,
        )
        copy.start()
        copies.append(copy)
    owner = dest[...]
    names = lax.broadcasted_iota(jnp.int32, (owners, per_row), 0)
    named = (names == owner).astype(jnp.float32)
    before = (
        lax.broadcasted_iota(jnp.int32, (per_row, per_row), 0)
        < lax.broadcasted_iota(jnp.int32, (per_row, per_row), 1)
    ).astype(jnp.float32)
    rank = jnp.dot(named, before, preferred_element_type=jnp.float32)
    slot = jnp.sum(rank * named, axis=0, keepdims=True)
    spot = owner.astype(jnp.float32) * capacity + slot
    rows = lax.broadcasted_iota(jnp.int32, (owners * capacity, per_row), 0).astype(jnp.float32)
    select = (rows == spot).astype(jnp.float32)
    total = parts[me]
    for copy in copies:
        copy.wait()
    for d in range(1, slab):
        total = total + arrived[d - 1]
    packed[...] = jnp.dot(
        select, total, precision=lax.Precision.HIGHEST, preferred_element_type=jnp.float32
    ).reshape(packed.shape)
    copies = []
    for d in range(1, owners):
        to = lax.rem(q + d, owners)
        copy = pltpu.make_async_remote_copy(
            src_ref=packed.at[to],
            dst_ref=out.at[q],
            send_sem=o_send.at[d - 1],
            recv_sem=o_recv.at[d - 1],
            device_id=(me, to),
            device_id_type=MESH,
        )
        copy.start()
        copies.append(copy)
    own = pltpu.make_async_copy(packed.at[q], out.at[q], own_sem)
    own.start()
    own.wait()
    for copy in copies:
        copy.wait()


def local(station_place, station_height, cell_weight, kept, dest):
    slab = lax.axis_size("slab")
    owners = lax.axis_size("sta")
    x_local, y_cells, z_cells = cell_weight.shape
    stations = station_place.shape[0]
    keep = kept.shape[2]
    lanes = 2 * z_cells
    per_row = stations * keep
    capacity = max(2, 3 * per_row // owners)
    chunk = 8
    ids = lax.all_gather(kept, "slab", axis=0, tiled=True).reshape(slab, per_row)
    sizes = (slab, stations, keep, x_local, y_cells, z_cells, chunk)
    pairs = stations // 2
    parts = pl.pallas_call(
        functools.partial(local_kernel, sizes),
        grid=(x_local // chunk,),
        out_shape=jax.ShapeDtypeStruct((slab, per_row, lanes), jnp.float32),
        in_specs=[
            pl.BlockSpec(memory_space=pltpu.SMEM),
            pl.BlockSpec(memory_space=pltpu.SMEM),
            pl.BlockSpec((chunk, y_cells, z_cells), lambda i: (i, 0, 0)),
            pl.BlockSpec((slab, per_row), lambda i: (0, 0)),
        ],
        out_specs=pl.BlockSpec((slab, per_row, lanes), lambda i: (0, 0, 0)),
        scratch_shapes=[
            pltpu.VMEM((pairs * x_local * y_cells, lanes), jnp.float32),
            pltpu.VMEM((chunk * y_cells, lanes), jnp.float32),
            pltpu.VMEM((pairs, y_cells // 8, 8, lanes), jnp.float32),
            pltpu.VMEM((slab, per_row), jnp.int32),
            pltpu.SMEM((slab, per_row), jnp.int32),
            pltpu.VMEM((2 * per_row, lanes), jnp.float32),
            pltpu.SemaphoreType.DMA,
        ],
        compiler_params=pltpu.CompilerParams(vmem_limit_bytes=48 * 2**20),
    )(station_place, station_height, cell_weight, ids)
    out = pl.pallas_call(
        functools.partial(send_kernel, (slab, owners, per_row, capacity)),
        out_shape=jax.ShapeDtypeStruct((owners, capacity, lanes), jnp.float32),
        in_specs=[pl.BlockSpec(memory_space=pltpu.VMEM)] * 2,
        out_specs=pl.BlockSpec(memory_space=pltpu.VMEM),
        scratch_shapes=[
            pltpu.VMEM((slab - 1, per_row, lanes), jnp.float32),
            pltpu.VMEM((owners, capacity, lanes), jnp.float32),
            pltpu.SemaphoreType.DMA((slab - 1,)),
            pltpu.SemaphoreType.DMA((slab - 1,)),
            pltpu.SemaphoreType.DMA((owners - 1,)),
            pltpu.SemaphoreType.DMA((owners - 1,)),
            pltpu.SemaphoreType.DMA,
        ],
        compiler_params=pltpu.CompilerParams(collective_id=0, has_side_effects=True),
    )(parts, dest.reshape(1, per_row))
    return out.reshape(1, 1, owners, capacity, lanes)


def solution(mesh):
    placed = (
        P("sta", None),
        P("sta"),
        P("slab", None, None),
        P("slab", "sta", None),
        P("slab", "sta", None, None),
    )
    return jax.shard_map(
        local,
        mesh=mesh,
        in_specs=placed,
        out_specs=P("slab", "sta", None, None, None),
        check_vma=False,
    )
```

```python
import functools

import jax
import jax.numpy as jnp
from jax import lax
from jax.experimental import pallas as pl
from jax.experimental.pallas import tpu as pltpu
from jax.sharding import PartitionSpec as P

kernel_scale = 32.0
MESH = pl.DeviceIdType.MESH


def log2(n):
    return n.bit_length() - 1


def row_plan(ids, j, me, slab, half, x_cells, y_cells):
    ls = log2(slab)
    a = ids >> log2(half)
    pair = j * half + (ids & (half - 1))
    here = jnp.zeros_like(a)
    factor = jnp.full(a.shape, x_cells ** -0.5, jnp.float32)
    m = 1
    while m < x_cells:
        e = log2(m)
        at = a >= m
        k = a - m
        norm = (m / x_cells) ** 0.5
        if m >= slab:
            sh = e - ls
            mine = (k >> sh) == me
            here = jnp.where(at, (m >> ls) + (k & ((1 << sh) - 1)), here)
            factor = jnp.where(at, jnp.where(mine, norm, 0.0), factor)
        else:
            sh = ls - e
            mine = k == (me >> sh)
            sign = norm * (1 - 2 * ((me >> (sh - 1)) & 1)).astype(jnp.float32)
            factor = jnp.where(at, jnp.where(mine, sign, 0.0), factor)
        m = m * 2
    ynorm = jnp.full(a.shape, y_cells ** -0.5, jnp.float32)
    m = 1
    while m < y_cells // 2:
        ynorm = jnp.where(pair >= m, (2 * m / y_cells) ** 0.5, ynorm)
        m = m * 2
    return here * y_cells + 2 * pair, factor * ynorm


def z_matrix(z_cells, t):
    z = lax.broadcasted_iota(jnp.int32, (2 * z_cells, 2 * z_cells), 0) & (z_cells - 1)
    lane = lax.broadcasted_iota(jnp.int32, (2 * z_cells, 2 * z_cells), 1)
    c = lane & (z_cells - 1)
    value = jnp.full(z.shape, z_cells ** -0.5, jnp.float32)
    m = 1
    while m < z_cells:
        w = log2(z_cells // m)
        k = c - m
        norm = (m / z_cells) ** 0.5
        hit = (z >> w) == k
        up = ((z >> (w - 1)) & 1) == 0
        value = jnp.where(c >= m, jnp.where(hit, jnp.where(up, norm, -norm), 0.0), value)
        m = m * 2
    return jnp.where((lane >> log2(z_cells)) == t, value, 0.0)


def tree(values):
    out = [None] * len(values)
    while len(values) > 1:
        half = len(values) // 2
        for k in range(half):
            out[half + k] = values[2 * k] - values[2 * k + 1]
        values = [values[2 * k] + values[2 * k + 1] for k in range(half)]
    out[0] = values[0]
    return out


GROUP = 4


def whole_kernel(
    sizes, place, height, w_ref, kept, dest, out,
    field, twice, table, select, others, rows_v, rows_s, taken, parts, arrived, packed,
    row_sem, i_send, i_recv, s_send, s_recv, o_send, o_recv, own_sem,
):
    slab, owners, stations, keep, x_local, y_cells, z_cells, chunk, capacity = sizes
    lanes = 2 * z_cells
    pairs = stations // 2
    x_cells = x_local * slab
    half = y_cells // slab // 2
    per_row = stations * keep
    runs = y_cells // 8
    step = pl.program_id(0)
    last = pl.num_programs(0) - 1
    me, q = lax.axis_index("slab"), lax.axis_index("sta")
    plane = x_local * y_cells
    left = lax.broadcasted_iota(jnp.int32, (8, lanes), 1) < z_cells
    zed = (lax.broadcasted_iota(jnp.int32, (8, lanes), 1) & (z_cells - 1)).astype(jnp.float32) + 0.5

    def two(pair, of):
        return jnp.where(left, of(2 * pair), of(2 * pair + 1))

    depths = [zed + two(p, lambda s: height[s]) for p in range(pairs)]

    def before(d):
        return lax.rem(me - d + slab, slab)

    def id_copy(d):
        return pltpu.make_async_remote_copy(
            src_ref=kept.at[0],
            dst_ref=others.at[d - 1],
            send_sem=i_send.at[d - 1],
            recv_sem=i_recv.at[d - 1],
            device_id=(lax.rem(me + d, slab), q),
            device_id_type=MESH,
        )

    def part_copy(d):
        return pltpu.make_async_remote_copy(
            src_ref=parts.at[d],
            dst_ref=arrived.at[d - 1],
            send_sem=s_send.at[d - 1],
            recv_sem=s_recv.at[d - 1],
            device_id=(before(d), q),
            device_id_type=MESH,
        )

    def out_copy(d):
        to = lax.rem(q + d, owners)
        return pltpu.make_async_remote_copy(
            src_ref=packed.at[to],
            dst_ref=out.at[q],
            send_sem=o_send.at[d - 1],
            recv_sem=o_recv.at[d - 1],
            device_id=(me, to),
            device_id_type=MESH,
        )

    def row_copy():
        return pltpu.make_async_copy(rows_v, rows_s, row_sem)

    @pl.when(step == 0)
    def _():
        barrier = pltpu.get_barrier_semaphore()
        for d in range(1, slab):
            pl.semaphore_signal(
                barrier, inc=1, device_id=(lax.rem(me + d, slab), q), device_id_type=MESH
            )
        for d in range(1, owners):
            pl.semaphore_signal(
                barrier, inc=1, device_id=(me, lax.rem(q + d, owners)), device_id_type=MESH
            )
        base = (lax.broadcasted_iota(jnp.int32, (8, lanes), 0) * runs).astype(jnp.float32) + 0.5
        for p in range(pairs):
            square = depths[p] * depths[p]
            north = base - two(p, lambda s: place[s, 1] * y_cells)
            for r in range(runs):
                n = north + float(r)
                table[p, r] = n * n + square
        owner = jnp.zeros((1, per_row), jnp.float32)
        for s in range(stations):
            spread = lax.broadcasted_iota(jnp.int32, (keep, per_row), 1) == (
                lax.broadcasted_iota(jnp.int32, (keep, per_row), 0) + s * keep
            )
            owner = owner + jnp.dot(
                dest[s].astype(jnp.float32), spread.astype(jnp.float32),
                preferred_element_type=jnp.float32,
            )
        names = lax.broadcasted_iota(jnp.int32, (owners, per_row), 0).astype(jnp.float32)
        named = (names == owner).astype(jnp.float32)
        earlier = (
            lax.broadcasted_iota(jnp.int32, (per_row, per_row), 0)
            < lax.broadcasted_iota(jnp.int32, (per_row, per_row), 1)
        ).astype(jnp.float32)
        rank = jnp.dot(named, earlier, preferred_element_type=jnp.float32)
        slot = jnp.sum(rank * named, axis=0, keepdims=True)
        spot = owner * capacity + slot
        rows = lax.broadcasted_iota(jnp.int32, (owners * capacity, per_row), 0).astype(jnp.float32)
        select[...] = (rows == spot).astype(jnp.float32)
        pl.semaphore_wait(barrier, slab + owners - 2)
        for d in range(1, slab):
            id_copy(d).start()

    @pl.when(step == last)
    def _():
        for d in range(1, slab):
            id_copy(d).wait()
        for d in range(slab):
            ids = kept[0] if d == 0 else others[d - 1]
            found, _ = row_plan(ids, before(d), me, slab, half, x_cells, y_cells)
            rows_v[d] = found
        row_copy().start()

    first = step * chunk
    for u in range(chunk):
        wide = w_ref[u]
        twice[pl.ds(u * y_cells, y_cells), :] = jnp.concatenate([wide, wide], axis=0).T

    def group(g, carry):
        x0 = first + g * GROUP
        for p in range(pairs):
            easts = []
            for u in range(GROUP):
                x = (me * x_local + x0 + u).astype(jnp.float32) + 0.5
                e = x - two(p, lambda s: place[s, 0] * x_cells)
                easts.append(e * e)

            def emit(level, run, values):
                if level is None:
                    start, stride = 0, 1
                else:
                    stride = runs >> level
                    start = (y_cells >> level) + run
                out = tree(values)
                for h in range(GROUP):
                    if h == 0:
                        xrow = x0 // GROUP
                    else:
                        m = 1 << log2(h)
                        xrow = x_local * m // GROUP + (x0 * m // GROUP) + (h - m)
                    at = p * plane + xrow * y_cells + start
                    if stride == 1:
                        field[pl.ds(at, 8), :] = out[h]
                    else:
                        field[pl.ds(at, 8, stride=stride), :] = out[h]

            stack = []
            for r in range(runs):
                t = table[p, r]
                values = []
                for u in range(GROUP):
                    inv = lax.rsqrt(t + easts[u])
                    w = twice[pl.ds((g * GROUP + u) * y_cells + r, 8, stride=runs), :]
                    values.append((w * inv) * (inv * inv))
                level, run = 0, r
                while stack and stack[-1][0] == level:
                    _, other = stack.pop()
                    level, run = level + 1, run >> 1
                    emit(level, run, [o - v for o, v in zip(other, values)])
                    values = [o + v for o, v in zip(other, values)]
                stack.append((level, values))
            emit(None, 0, stack[0][1])
        return carry

    lax.fori_loop(0, chunk // GROUP, group, 0)

    @pl.when(step == last)
    def _():
        coarse = x_local // GROUP

        def finish_x(tile, carry):
            for p in range(pairs):
                at = [p * plane + x * y_cells + tile * 8 for x in range(coarse)]
                values = tree([field[pl.ds(pl.multiple_of(a, 8), 8), :] for a in at])
                for a, v in zip(at, values):
                    field[pl.ds(pl.multiple_of(a, 8), 8), :] = v
            return carry

        lax.fori_loop(0, runs, finish_x, 0)

        def finish_y(block, carry):
            for p in range(pairs):
                at = p * plane + block * (8 * y_cells)
                values = tree([field[pl.ds(at + i, 8, stride=y_cells), :] for i in range(8)])
                for i in range(8):
                    field[pl.ds(at + i, 8, stride=y_cells), :] = values[i]
            return carry

        lax.fori_loop(0, x_local // 8, finish_y, 0)
        even, odd = z_matrix(z_cells, 0), z_matrix(z_cells, 1)
        eye = lax.broadcasted_iota(jnp.int32, (keep, keep), 0) == lax.broadcasted_iota(
            jnp.int32, (keep, keep), 1
        )
        side = lax.broadcasted_iota(jnp.int32, (1, lanes), 1) < z_cells
        row_copy().wait()

        def part(d, ids):
            for s in range(stations):
                for i in range(keep):
                    k = s * keep + i
                    at = (s // 2) * plane + rows_s[d, s, i]
                    taken[2 * k : 2 * k + 2, :] = field[pl.ds(at, 2), :]
            _, factor = row_plan(ids, before(d), me, slab, half, x_cells, y_cells)
            scales = []
            for s in range(stations):
                z_part = kernel_scale * depths[s // 2][0:1, :]
                z_part = jnp.where(side if s % 2 == 0 else jnp.logical_not(side), z_part, 0.0)
                column = jnp.sum(jnp.where(eye, factor[s : s + 1, :], 0.0), axis=1, keepdims=True)
                scales.append(column * z_part)
            scale = jnp.concatenate(scales, axis=0)
            x_even = taken[pl.ds(0, per_row, stride=2), :] * scale
            x_odd = taken[pl.ds(1, per_row, stride=2), :] * scale
            return jnp.dot(
                x_even, even, precision=lax.Precision.HIGHEST, preferred_element_type=jnp.float32
            ) + jnp.dot(x_odd, odd, precision=lax.Precision.HIGHEST, preferred_element_type=jnp.float32)

        def send_part(d, carry):
            parts[d] = part(d, others[d - 1])
            part_copy(d).start()
            return carry

        lax.fori_loop(1, slab, send_part, 0)
        total = part(0, kept[0])
        for d in range(1, slab):
            part_copy(d).wait()
            total = total + arrived[d - 1]
        packed[...] = jnp.dot(
            select[...], total, precision=lax.Precision.HIGHEST, preferred_element_type=jnp.float32
        ).reshape(packed.shape)
        for d in range(1, owners):
            out_copy(d).start()
        own = pltpu.make_async_copy(packed.at[q], out.at[q], own_sem)
        own.start()
        own.wait()
        for d in range(1, owners):
            out_copy(d).wait()


def local(station_place, station_height, cell_weight, kept, dest):
    slab = lax.axis_size("slab")
    owners = lax.axis_size("sta")
    x_local, y_cells, z_cells = cell_weight.shape
    stations = station_place.shape[0]
    keep = kept.shape[2]
    lanes = 2 * z_cells
    per_row = stations * keep
    capacity = max(2, 3 * per_row // owners)
    chunk = 8
    sizes = (slab, owners, stations, keep, x_local, y_cells, z_cells, chunk, capacity)
    pairs = stations // 2
    dma = pltpu.SemaphoreType.DMA
    out = pl.pallas_call(
        functools.partial(whole_kernel, sizes),
        grid=(x_local // chunk,),
        out_shape=jax.ShapeDtypeStruct((owners, capacity, lanes), jnp.float32),
        in_specs=[
            pl.BlockSpec(memory_space=pltpu.SMEM),
            pl.BlockSpec(memory_space=pltpu.SMEM),
            pl.BlockSpec((chunk, z_cells, y_cells), lambda i: (i, 0, 0)),
            pl.BlockSpec(memory_space=pltpu.VMEM),
            pl.BlockSpec(memory_space=pltpu.VMEM),
        ],
        out_specs=pl.BlockSpec(memory_space=pl.ANY),
        scratch_shapes=[
            pltpu.VMEM((pairs * x_local * y_cells, lanes), jnp.float32),
            pltpu.VMEM((chunk * y_cells, lanes), jnp.float32),
            pltpu.VMEM((pairs, y_cells // 8, 8, lanes), jnp.float32),
            pltpu.VMEM((owners * capacity, per_row), jnp.float32),
            pltpu.VMEM((slab - 1, stations, keep), jnp.int32),
            pltpu.VMEM((slab, stations, keep), jnp.int32),
            pltpu.SMEM((slab, stations, keep), jnp.int32),
            pltpu.VMEM((2 * per_row, lanes), jnp.float32),
            pltpu.VMEM((slab, per_row, lanes), jnp.float32),
            pltpu.VMEM((slab - 1, per_row, lanes), jnp.float32),
            pltpu.VMEM((owners, capacity, lanes), jnp.float32),
            dma,
            dma((slab - 1,)),
            dma((slab - 1,)),
            dma((slab - 1,)),
            dma((slab - 1,)),
            dma((owners - 1,)),
            dma((owners - 1,)),
            dma,
        ],
        compiler_params=pltpu.CompilerParams(
            collective_id=0, has_side_effects=True, vmem_limit_bytes=60 * 1024 * 1024
        ),
    )(
        station_place,
        station_height,
        jnp.transpose(cell_weight, (0, 2, 1)),
        kept,
        jnp.transpose(dest, (0, 1, 3, 2)).reshape(stations, 1, keep),
    )
    return out.reshape(1, 1, owners, capacity, lanes)


def solution(mesh):
    placed = (
        P("sta", None),
        P("sta"),
        P("slab", None, None),
        P("slab", "sta", None),
        P("slab", "sta", None, None),
    )
    return jax.shard_map(
        local,
        mesh=mesh,
        in_specs=placed,
        out_specs=P("slab", "sta", None, None, None),
        check_vma=False,
    )
```
